32 devices in a mesh: layer: 8 (over y, x, core), dp: 4 (over z).
Axes of the slice: x: 2, y: 2, z: 4, core: 2. Of those that a mesh axis runs over, the one named last changes fastest.
Arguments:
- initial: float32 [256, 1024], P('dp'), may hold values from -6 to 6
- norm_gains: float32 [32, 1024], P('layer'), may hold values from 0.25 to 1.75
- first_weights: bfloat16 [32, 1024, 2048], P('layer'), may hold values from -0.1875 to 0.1875
- second_weights: bfloat16 [32, 2048, 1024], P('layer'), may hold values from -0.046875 to 0.046875
Outputs:
- layer_states: float32 [32, 256, 1024], P('layer', 'dp')
- residual_ratios: float32 [7], replicated
- coarse_defects_four: float32 [32, 256, 1024], P('layer', 'dp')
- coarse_defects_sixteen: float32 [32, 256, 1024], P('layer', 'dp')
The draws below stay inside these ranges and needn't reach their ends.
All inputs are finite; a program needn't handle non-finite values.
Results may differ from the reference program's by a relative error of at most 0.02.
Values sent between devices are 32-bit elements; how exact they have to be, the bound alone decides.
A program may use at most 128 MiB of HBM per device.

```python
import jax
import jax.numpy as jnp
from jax import lax

D = 1024
FF = 2048
LAYERS = 32
TOKENS = 256


def steps_of(own_key, shape, cuts, least, high):
    level, own = 1.0, jax.random.fold_in(own_key, 6)
    for position, parts in cuts:
        steps = jnp.exp(jax.random.uniform(jax.random.fold_in(own, position), (parts,), jnp.float32, least / len(cuts), high / len(cuts)))
        level = level * jnp.repeat(steps, shape[position] // parts).reshape([-1 if axis == position else 1 for axis in range(len(shape))])
    return level


def noise(own_key, shape, scale, bound, cuts=(), kind=jnp.bfloat16):
    result = jax.random.normal(own_key, shape, jnp.float32) * scale
    if len(cuts) > 0:
        result = steps_of(own_key, shape, cuts, -0.22, 0.18) * result
    return jnp.clip(result, min=-bound, max=bound).astype(kind)


def setup_inputs(seed: int = 0) -> dict:
    key_of = jax.random.split(jax.random.key(seed), 5)
    initial = noise(key_of[0], (TOKENS, D), 1.0, 6.0, ((0, 4),), jnp.float32)
    norm_gains = jnp.clip(1.0 + 0.15 * jax.random.normal(key_of[1], (LAYERS, D), jnp.float32), 0.25, 1.75)
    first_weights = noise(key_of[2], (LAYERS, D, FF), D ** -0.5, 0.1875, ((0, 8),))
    second_weights = noise(key_of[3], (LAYERS, FF, D), (7 * FF) ** -0.5, 0.046875, ((0, 8),))
    return {"initial": initial, "norm_gains": norm_gains, "first_weights": first_weights, "second_weights": second_weights}


epsilon = 1e-06

def branch(row_block, weight_in, weight_out, gain_row):
    mean_square = lax.optimization_barrier(jnp.mean(row_block * row_block, axis=-1, keepdims=True))
    normed = (row_block * lax.rsqrt(mean_square + epsilon) * gain_row).astype(jnp.bfloat16)
    hidden = jax.nn.gelu(jnp.dot(normed, weight_in, preferred_element_type=jnp.float32), approximate=True).astype(jnp.bfloat16)
    return jnp.dot(hidden, weight_out, preferred_element_type=jnp.float32)

def reference(initial, norm_gains, first_weights, second_weights):
    layer_total = LAYERS
    history = [initial] * (layer_total + 1)

    def propagate(point, values, spacing):
        return values + spacing * branch(values, first_weights[point - 1], second_weights[point - 1], norm_gains[point - 1])

    def relaxation(spacing, residues, right_side):
        for residue in residues:
            for point in range(spacing, layer_total + 1, spacing):
                if point % (4 * spacing) == residue:
                    updated = propagate(point, history[point - spacing], spacing)
                    if right_side is not None:
                        updated = updated + right_side[point]
                    history[point] = updated

    def restrict(spacing, right_side):
        coarse = {}
        gap_sums = []
        step_sums = []
        for point in range(4 * spacing, layer_total + 1, 4 * spacing):
            before = history[point - spacing]
            update = branch(before, first_weights[point - 1], second_weights[point - 1], norm_gains[point - 1])
            fine_value = before + spacing * update
            if right_side is not None:
                fine_value = fine_value + right_side[point]
            coarse[point] = fine_value - propagate(point, history[point - 4 * spacing], 4 * spacing)
            gap = fine_value - history[point]
            gap_sums.append(jnp.sum(gap * gap))
            step_sums.append(jnp.sum(update * update))
        return (coarse, gap_sums, step_sums)

    def defects(spacing):
        rows = []
        for point in range(1, layer_total + 1):
            if point >= spacing:
                rows.append(history[point] - propagate(point, history[point - spacing], spacing))
            else:
                rows.append(jnp.zeros_like(initial))
        return jnp.stack(rows)
    relaxation(1, (1, 2, 3), None)
    relaxation(1, (0,), None)
    relaxation(1, (1, 2, 3), None)
    rhs_one, gap_sums, step_sums = restrict(1, None)
    relaxation(4, (4, 8, 12), rhs_one)
    rhs_two, unused_gaps, unused_steps = restrict(4, rhs_one)
    for point in range(16, layer_total + 1, 16):
        history[point] = propagate(point, history[point - 16], 16) + rhs_two[point]
    relaxation(4, (4, 8, 12), rhs_one)
    relaxation(1, (1, 2, 3), None)
    layer_states = jnp.stack(history[1:])
    residual_ratios = jnp.sqrt(jnp.stack(gap_sums[1:]) / (jnp.stack(step_sums[1:]) + epsilon))
    defects_four = defects(4)
    defects_sixteen = defects(16)
    return (layer_states, residual_ratios, defects_four, defects_sixteen)
```

```python
import jax
import jax.numpy as jnp
from jax import lax
from jax.sharding import PartitionSpec as P

epsilon = 1e-06


def shifted(block, axis, distance):
    devices = range(lax.axis_size(axis))
    route = [(i - distance, i) for i in devices if i - distance in devices]
    return lax.ppermute(block, axis, route)


def branch(row_block, weight_in, weight_out, gain_row):
    mean_square = jnp.mean(row_block * row_block, axis=-1, keepdims=True)
    normed = (row_block * lax.rsqrt(mean_square + epsilon) * gain_row).astype(jnp.bfloat16)
    hidden = jax.nn.gelu(
        jnp.dot(normed, weight_in, preferred_element_type=jnp.float32), approximate=True
    ).astype(jnp.bfloat16)
    return jnp.dot(hidden, weight_out, preferred_element_type=jnp.float32)


def local(initial, norm_gains, first_weights, second_weights):
    slot_count = first_weights.shape[0]
    sections = lax.axis_size("layer")
    layer_total = slot_count * sections
    norm_count = layer_total // 4 - 1
    first_point = lax.axis_index("layer") * slot_count
    points = first_point + jnp.arange(slot_count, dtype=jnp.int32) + 1
    spacings = (1, 4, 16)

    def shaped(flags, rank):
        return flags.reshape((slot_count,) + (1,) * (rank - 1))

    def previous(values, level_index):
        spacing = spacings[level_index]
        if spacing >= slot_count:
            portion = values
            distance = spacing // slot_count
        else:
            portion = values[slot_count - spacing :]
            distance = 1
        if level_index == 0:
            arrived = shifted(portion, "layer", distance)
        elif level_index == 1:
            arrived = shifted(portion, "layer", distance)
        else:
            arrived = shifted(portion, "layer", distance)
        if spacing < slot_count:
            arrived = jnp.concatenate([arrived, values[: slot_count - spacing]], axis=0)
        return arrived

    def incoming(values, level_index, anchor):
        arrived = previous(values, level_index)
        from_anchor = shaped(points - spacings[level_index] == 0, values.ndim)
        return jnp.where(from_anchor, anchor, arrived)

    def advance(before, level_index, active, right_side):
        factor = float(spacings[level_index])
        results = []
        for slot in range(slot_count):

            def advance_compute(values, source, slot=slot):
                return (
                    values
                    + factor
                    * branch(values, first_weights[slot], second_weights[slot], norm_gains[slot])
                    + source
                )

            def advance_unchanged(values, source):
                return values

            source = right_side[slot] if right_side is not None else jnp.zeros_like(before[slot])
            results.append(
                lax.cond(active[slot], advance_compute, advance_unchanged, before[slot], source)
            )
        return jnp.stack(results)

    def relaxation(current, level_index, residues, right_side, anchor):
        modulus = 4 * spacings[level_index]
        for residue in residues:
            before = incoming(current, level_index, anchor)
            active = points % modulus == residue
            current = jnp.where(
                shaped(active, 3), advance(before, level_index, active, right_side), current
            )
        return (current, None)

    def restrict(current, level_index, right_side, anchor):
        spacing = spacings[level_index]
        factor = float(spacing)
        wide_factor = float(4 * spacing)
        before = incoming(current, level_index, anchor)
        far_state = incoming(current, level_index + 1, anchor)
        active = points % (4 * spacing) == 0
        row_count = current.shape[1]
        coarse_list = []
        gap_list = []
        step_list = []
        for slot in range(slot_count):

            def restrict_compute(near, distant, held, source, slot=slot):
                update = branch(
                    jnp.concatenate([near, distant], axis=0),
                    first_weights[slot],
                    second_weights[slot],
                    norm_gains[slot],
                )
                near_term = update[:row_count]
                fine_value = near + factor * near_term + source
                coarse = fine_value - (distant + wide_factor * update[row_count:])
                gap = fine_value - held
                return (coarse, jnp.sum(gap * gap), jnp.sum(near_term * near_term))

            def restrict_unchanged(near, distant, held, source):
                nothing = jnp.zeros((), near.dtype)
                return (jnp.zeros_like(near), nothing, nothing)

            source = right_side[slot] if right_side is not None else jnp.zeros_like(before[slot])
            coarse, gap_sum, step_sum = lax.cond(
                active[slot],
                restrict_compute,
                restrict_unchanged,
                before[slot],
                far_state[slot],
                current[slot],
                source,
            )
            coarse_list.append(coarse)
            gap_list.append(gap_sum)
            step_list.append(step_sum)
        return (jnp.stack(coarse_list), jnp.stack(gap_list), jnp.stack(step_list))

    def defects(current, level_index, anchor):
        spacing = spacings[level_index]
        factor = float(spacing)
        before = incoming(current, level_index, anchor)
        stepped = []
        for slot in range(slot_count):
            stepped.append(
                before[slot]
                + factor
                * branch(before[slot], first_weights[slot], second_weights[slot], norm_gains[slot])
            )
        valid = shaped(points >= spacing, 3)
        return jnp.where(valid, current - jnp.stack(stepped), 0.0)

    def multigrid_cycle(anchor):
        current = jnp.broadcast_to(anchor, (slot_count,) + anchor.shape)
        current, unused = relaxation(current, 0, (1, 2, 3), None, anchor)
        current, unused = relaxation(current, 0, (0,), None, anchor)
        current, carried = relaxation(current, 0, (1, 2, 3), None, anchor)
        rhs_one, gap_sums, step_sums = restrict(current, 0, None, anchor)
        current, carried = relaxation(current, 1, (4, 8, 12), rhs_one, anchor)
        rhs_two, unused_gaps, unused_steps = restrict(current, 1, rhs_one, anchor)
        for coarse_step in range(1, layer_total // 16 + 1):
            active = points == 16 * coarse_step
            before = incoming(current, 2, anchor)
            current = jnp.where(shaped(active, 3), advance(before, 2, active, rhs_two), current)
        current, unused = relaxation(current, 1, (4, 8, 12), rhs_one, anchor)
        current, unused = relaxation(current, 0, (1, 2, 3), None, anchor)
        defects_four = defects(current, 1, anchor)
        defects_sixteen = defects(current, 2, anchor)
        return (current, gap_sums, step_sums, defects_four, defects_sixteen)

    portions = [initial]
    outcomes = [multigrid_cycle(portion) for portion in portions]
    layer_states = jnp.concatenate([outcome[0] for outcome in outcomes], axis=1)
    defects_four = jnp.concatenate([outcome[3] for outcome in outcomes], axis=1)
    defects_sixteen = jnp.concatenate([outcome[4] for outcome in outcomes], axis=1)
    gap_sums = outcomes[0][1]
    step_sums = outcomes[0][2]
    counted = (points % 4 == 0) & (points >= 8)
    entry_index = points // 4 - 2
    one_hot = (
        (jnp.arange(norm_count, dtype=jnp.int32)[None, :] == entry_index[:, None])
        & counted[:, None]
    ).astype(jnp.float32)
    gap_vector = jnp.sum(gap_sums[:, None] * one_hot, axis=0)
    step_vector = jnp.sum(step_sums[:, None] * one_hot, axis=0)
    gap_total, step_total = lax.psum((gap_vector, step_vector), ("layer", "dp"))
    residual_ratios = jnp.sqrt(gap_total / (step_total + epsilon))
    return (layer_states, residual_ratios, defects_four, defects_sixteen)


def local_quads(initial, norm_gains, first_weights, second_weights):
    sections = lax.axis_size("layer")
    blocks = sections // 4
    here = lax.axis_index("layer")
    place = here % 4
    rows = initial.shape[0]

    def moved(slot, *states):
        stacked = states[0] if len(states) == 1 else jnp.concatenate(states, axis=0)
        return branch(stacked, first_weights[slot], second_weights[slot], norm_gains[slot])

    def near(values):
        return jnp.where(here == 0, initial, shifted(values, "layer", 1))

    def distant(values):
        return jnp.where(here == 3, initial, shifted(values, "layer", 4))

    state = initial
    for slot in range(4):
        state = state + moved(slot, state)
    point = state
    left = near(point)
    far = distant(point)
    state = left
    for slot in range(3):
        state = state + moved(slot, state)
    update = moved(3, state, left, far)
    near_term = update[:rows]
    fine = state + near_term
    rhs_one = fine - (left + 4.0 * update[rows : 2 * rows])
    far_step = far + 16.0 * update[2 * rows :]
    gap = fine - point
    gap_sum = jnp.sum(gap * gap)
    step_sum = jnp.sum(near_term * near_term)

    point = jnp.where(place == 0, fine, point)
    for residue in (1, 2, 3):
        before = near(point)
        stepped = before + 4.0 * moved(3, before) + rhs_one
        point = jnp.where(place == residue, stepped, point)
    rhs_two = point - far_step

    wide = place == 3
    factor = jnp.where(wide, 16.0, 4.0)
    source = jnp.where(wide, rhs_two, rhs_one)
    for block in range(1, blocks):
        before = jnp.where(wide, distant(point), near(point))
        stepped = before + factor * moved(3, before) + source
        point = jnp.where((here == 4 * block) | (here == 4 * block + 3), stepped, point)
    for residue in (1, 2):
        before = near(point)
        stepped = before + 4.0 * moved(3, before) + rhs_one
        point = jnp.where(place == residue, stepped, point)

    left = near(point)
    far = distant(point)
    state = left
    states = []
    for slot in range(3):
        state = state + moved(slot, state)
        states.append(state)
    states.append(point)
    lefts = [shifted(s, "layer", 1) for s in states[:3]] + [left]
    fars = [shifted(s, "layer", 4) for s in states[:3]] + [far]
    fours = []
    sixteens = []
    for slot in range(4):
        update = moved(slot, lefts[slot], fars[slot])
        fours.append(states[slot] - (lefts[slot] + 4.0 * update[:rows]))
        sixteens.append(states[slot] - (fars[slot] + 16.0 * update[rows:]))
    points = here * 4 + jnp.arange(4, dtype=jnp.int32) + 1
    defects_four = jnp.where((points >= 4)[:, None, None], jnp.stack(fours), 0.0)
    defects_sixteen = jnp.where((points >= 16)[:, None, None], jnp.stack(sixteens), 0.0)
    one_hot = (jnp.arange(sections - 1) == here - 1).astype(jnp.float32)
    gap_total, step_total = lax.psum((gap_sum * one_hot, step_sum * one_hot), ("layer", "dp"))
    ratios = jnp.sqrt(gap_total / (step_total + epsilon))
    return (jnp.stack(states), ratios, defects_four, defects_sixteen)


def chosen(initial, norm_gains, first_weights, second_weights):
    quads = first_weights.shape[0] == 4 and lax.axis_size("layer") % 4 == 0
    return (local_quads if quads else local)(initial, norm_gains, first_weights, second_weights)


def solution(mesh):
    placed = (P("dp", None), P("layer", None), P("layer", None, None), P("layer", None, None))
    return jax.shard_map(
        chosen,
        mesh=mesh,
        in_specs=placed,
        out_specs=(P("layer", "dp", None), P(), P("layer", "dp", None), P("layer", "dp", None)),
        check_vma=False,
    )
```

```python
import jax
import jax.numpy as jnp
from jax import lax
from jax.experimental import pallas as pl
from jax.experimental.pallas import tpu as pltpu
from jax.sharding import PartitionSpec as P

epsilon = 1e-06


def shifted(block, axis, distance):
    devices = range(lax.axis_size(axis))
    route = [(i - distance, i) for i in devices if i - distance in devices]
    return lax.ppermute(block, axis, route)


def branch(row_block, weight_in, weight_out, gain_row):
    mean_square = jnp.mean(row_block * row_block, axis=-1, keepdims=True)
    normed = (row_block * lax.rsqrt(mean_square + epsilon) * gain_row).astype(jnp.bfloat16)
    hidden = jax.nn.gelu(
        jnp.dot(normed, weight_in, preferred_element_type=jnp.float32), approximate=True
    ).astype(jnp.bfloat16)
    return jnp.dot(hidden, weight_out, preferred_element_type=jnp.float32)


def local(initial, norm_gains, first_weights, second_weights):
    slot_count = first_weights.shape[0]
    sections = lax.axis_size("layer")
    layer_total = slot_count * sections
    norm_count = layer_total // 4 - 1
    first_point = lax.axis_index("layer") * slot_count
    points = first_point + jnp.arange(slot_count, dtype=jnp.int32) + 1
    spacings = (1, 4, 16)

    def shaped(flags, rank):
        return flags.reshape((slot_count,) + (1,) * (rank - 1))

    def previous(values, level_index):
        spacing = spacings[level_index]
        if spacing >= slot_count:
            portion = values
            distance = spacing // slot_count
        else:
            portion = values[slot_count - spacing :]
            distance = 1
        if level_index == 0:
            arrived = shifted(portion, "layer", distance)
        elif level_index == 1:
            arrived = shifted(portion, "layer", distance)
        else:
            arrived = shifted(portion, "layer", distance)
        if spacing < slot_count:
            arrived = jnp.concatenate([arrived, values[: slot_count - spacing]], axis=0)
        return arrived

    def incoming(values, level_index, anchor):
        arrived = previous(values, level_index)
        from_anchor = shaped(points - spacings[level_index] == 0, values.ndim)
        return jnp.where(from_anchor, anchor, arrived)

    def advance(before, level_index, active, right_side):
        factor = float(spacings[level_index])
        results = []
        for slot in range(slot_count):

            def advance_compute(values, source, slot=slot):
                return (
                    values
                    + factor
                    * branch(values, first_weights[slot], second_weights[slot], norm_gains[slot])
                    + source
                )

            def advance_unchanged(values, source):
                return values

            source = right_side[slot] if right_side is not None else jnp.zeros_like(before[slot])
            results.append(
                lax.cond(active[slot], advance_compute, advance_unchanged, before[slot], source)
            )
        return jnp.stack(results)

    def relaxation(current, level_index, residues, right_side, anchor):
        modulus = 4 * spacings[level_index]
        for residue in residues:
            before = incoming(current, level_index, anchor)
            active = points % modulus == residue
            current = jnp.where(
                shaped(active, 3), advance(before, level_index, active, right_side), current
            )
        return (current, None)

    def restrict(current, level_index, right_side, anchor):
        spacing = spacings[level_index]
        factor = float(spacing)
        wide_factor = float(4 * spacing)
        before = incoming(current, level_index, anchor)
        far_state = incoming(current, level_index + 1, anchor)
        active = points % (4 * spacing) == 0
        row_count = current.shape[1]
        coarse_list = []
        gap_list = []
        step_list = []
        for slot in range(slot_count):

            def restrict_compute(near, distant, held, source, slot=slot):
                update = branch(
                    jnp.concatenate([near, distant], axis=0),
                    first_weights[slot],
                    second_weights[slot],
                    norm_gains[slot],
                )
                near_term = update[:row_count]
                fine_value = near + factor * near_term + source
                coarse = fine_value - (distant + wide_factor * update[row_count:])
                gap = fine_value - held
                return (coarse, jnp.sum(gap * gap), jnp.sum(near_term * near_term))

            def restrict_unchanged(near, distant, held, source):
                nothing = jnp.zeros((), near.dtype)
                return (jnp.zeros_like(near), nothing, nothing)

            source = right_side[slot] if right_side is not None else jnp.zeros_like(before[slot])
            coarse, gap_sum, step_sum = lax.cond(
                active[slot],
                restrict_compute,
                restrict_unchanged,
                before[slot],
                far_state[slot],
                current[slot],
                source,
            )
            coarse_list.append(coarse)
            gap_list.append(gap_sum)
            step_list.append(step_sum)
        return (jnp.stack(coarse_list), jnp.stack(gap_list), jnp.stack(step_list))

    def defects(current, level_index, anchor):
        spacing = spacings[level_index]
        factor = float(spacing)
        before = incoming(current, level_index, anchor)
        stepped = []
        for slot in range(slot_count):
            stepped.append(
                before[slot]
                + factor
                * branch(before[slot], first_weights[slot], second_weights[slot], norm_gains[slot])
            )
        valid = shaped(points >= spacing, 3)
        return jnp.where(valid, current - jnp.stack(stepped), 0.0)

    def multigrid_cycle(anchor):
        current = jnp.broadcast_to(anchor, (slot_count,) + anchor.shape)
        current, unused = relaxation(current, 0, (1, 2, 3), None, anchor)
        current, unused = relaxation(current, 0, (0,), None, anchor)
        current, carried = relaxation(current, 0, (1, 2, 3), None, anchor)
        rhs_one, gap_sums, step_sums = restrict(current, 0, None, anchor)
        current, carried = relaxation(current, 1, (4, 8, 12), rhs_one, anchor)
        rhs_two, unused_gaps, unused_steps = restrict(current, 1, rhs_one, anchor)
        for coarse_step in range(1, layer_total // 16 + 1):
            active = points == 16 * coarse_step
            before = incoming(current, 2, anchor)
            current = jnp.where(shaped(active, 3), advance(before, 2, active, rhs_two), current)
        current, unused = relaxation(current, 1, (4, 8, 12), rhs_one, anchor)
        current, unused = relaxation(current, 0, (1, 2, 3), None, anchor)
        defects_four = defects(current, 1, anchor)
        defects_sixteen = defects(current, 2, anchor)
        return (current, gap_sums, step_sums, defects_four, defects_sixteen)

    portions = [initial]
    outcomes = [multigrid_cycle(portion) for portion in portions]
    layer_states = jnp.concatenate([outcome[0] for outcome in outcomes], axis=1)
    defects_four = jnp.concatenate([outcome[3] for outcome in outcomes], axis=1)
    defects_sixteen = jnp.concatenate([outcome[4] for outcome in outcomes], axis=1)
    gap_sums = outcomes[0][1]
    step_sums = outcomes[0][2]
    counted = (points % 4 == 0) & (points >= 8)
    entry_index = points // 4 - 2
    one_hot = (
        (jnp.arange(norm_count, dtype=jnp.int32)[None, :] == entry_index[:, None])
        & counted[:, None]
    ).astype(jnp.float32)
    gap_vector = jnp.sum(gap_sums[:, None] * one_hot, axis=0)
    step_vector = jnp.sum(step_sums[:, None] * one_hot, axis=0)
    gap_total, step_total = lax.psum((gap_vector, step_vector), ("layer", "dp"))
    residual_ratios = jnp.sqrt(gap_total / (step_total + epsilon))
    return (layer_states, residual_ratios, defects_four, defects_sixteen)


def coarse_kernel(
    sections, copies,
    initial, start, rhs_one, far_step, tile, gain, w_in, w_out,
    point, left, far, totals,
    cur, slots, ends, normed, total, across, along, summed,
    send, arrive, end_arrive, across_send, across_arrive, along_send, along_arrive,
):
    here = lax.axis_index("layer")
    depth = lax.axis_index("dp")
    blocks = sections // 4
    wide_end = blocks + 2
    rounds = wide_end + 2
    ff = w_in.shape[2]
    width = ff // 4

    def to(layer, dp):
        return dict(device_id=(layer, dp), device_id_type=pl.DeviceIdType.MESH)

    cur[...] = start[...]
    across[depth] = tile[...]

    barrier = pltpu.get_barrier_semaphore()
    for k in range(1, sections):
        pl.semaphore_signal(barrier, inc=1, **to(lax.rem(here + k, sections), depth))
    for k in range(1, copies):
        pl.semaphore_signal(barrier, inc=1, **to(here, lax.rem(depth + k, copies)))
    pl.semaphore_wait(barrier, sections + copies - 2)

    def across_copy(k):
        return pltpu.make_async_remote_copy(
            src_ref=tile, dst_ref=across.at[depth],
            send_sem=across_send.at[k - 1], recv_sem=across_arrive.at[k - 1],
            **to(here, lax.rem(depth + k, copies)),
        )

    for k in range(1, copies):
        across_copy(k).start()

    def wide(d, r):
        return (r >= 3) & (r < wide_end) & (d == 4 * (r - 2) + 3)

    def receives(d, r):
        early = (r < 3) & (lax.rem(d, 4) == r + 1)
        middle = (r >= 3) & (r < wide_end) & ((d == 4 * (r - 2)) | (d == 4 * (r - 2) + 3))
        late = (r >= wide_end) & (lax.rem(d, 4) == r - wide_end + 1) & (d >= 4)
        return early | middle | late

    def hop(r, distance):
        return pltpu.make_async_remote_copy(
            src_ref=cur, dst_ref=slots.at[r], send_sem=send.at[distance // 4],
            recv_sem=arrive.at[r], **to(lax.rem(here + distance, sections), depth),
        )

    def step(r, carry):
        one = (here + 1 < sections) & receives(here + 1, r) & jnp.logical_not(wide(here + 1, r))
        four = (here + 4 < sections) & wide(here + 4, r)

        @pl.when(one)
        def _():
            hop(r, 1).start()

        @pl.when(four)
        def _():
            hop(r, 4).start()

        @pl.when(one)
        def _():
            hop(r, 1).wait_send()

        @pl.when(four)
        def _():
            hop(r, 4).wait_send()

        @pl.when(receives(here, r))
        def _():
            hop(r, 1).wait_recv()
            before = slots[r]
            mean_square = jnp.mean(before * before, axis=-1, keepdims=True)
            normed[...] = (before * lax.rsqrt(mean_square + epsilon) * gain[...]).astype(
                jnp.bfloat16
            )
            total[...] = jnp.zeros_like(total)

            def part(i, c):
                cols = pl.ds(pl.multiple_of(i * width, width), width)
                hidden = jax.nn.gelu(
                    jnp.dot(normed[...], w_in[0, :, cols], preferred_element_type=jnp.float32),
                    approximate=True,
                ).astype(jnp.bfloat16)
                total[...] += jnp.dot(
                    hidden, w_out[0, cols, :], preferred_element_type=jnp.float32
                )
                return c

            lax.fori_loop(0, 4, part, 0)
            is_wide = wide(here, r)

            @pl.when(is_wide)
            def _():
                cur[...] = slots[r] + 16.0 * total[...] + (cur[...] - far_step[...])

            @pl.when(jnp.logical_not(is_wide))
            def _():
                cur[...] = slots[r] + 4.0 * total[...] + rhs_one[...]

        return carry

    lax.fori_loop(0, rounds, step, 0)

    def last(distance):
        return pltpu.make_async_remote_copy(
            src_ref=cur, dst_ref=ends.at[distance // 4], send_sem=send.at[distance // 4],
            recv_sem=end_arrive.at[distance // 4],
            **to(lax.rem(here + distance, sections), depth),
        )

    for distance in (1, 4):

        @pl.when(here + distance < sections)
        def _(distance=distance):
            last(distance).start()

    for k in range(1, copies):
        across_copy(k).wait()
    gathered = across[0]
    for k in range(1, copies):
        gathered = gathered + across[k]
    summed[...] = gathered

    def along_copy(k):
        return pltpu.make_async_remote_copy(
            src_ref=summed, dst_ref=along.at[k - 1],
            send_sem=along_send.at[k - 1], recv_sem=along_arrive.at[k - 1],
            **to(lax.rem(here + k, sections), depth),
        )

    for k in range(1, sections):
        along_copy(k).start()
    point[...] = cur[...]
    for distance, out, edge in ((1, left, 1), (4, far, 4)):

        @pl.when(here + distance < sections)
        def _(distance=distance):
            last(distance).wait_send()

        @pl.when(here >= edge)
        def _(distance=distance, out=out):
            last(distance).wait_recv()
            out[...] = ends[distance // 4]

        @pl.when(here < edge)
        def _(out=out):
            out[...] = initial[...]

    result = summed[...]
    for k in range(1, sections):
        along_copy(k).wait()
        result = result + along[k - 1]
    totals[...] = result


def coarse(initial, start, rhs_one, far_step, tile, gain, first_weights, second_weights):
    sections = lax.axis_size("layer")
    copies = lax.axis_size("dp")
    rounds = sections // 4 + 4
    shape = initial.shape
    d, ff = first_weights.shape[1:]
    whole = pl.BlockSpec(shape, lambda i: (0, 0))
    small = pl.BlockSpec((8, 128), lambda i: (0, 0))
    state = jax.ShapeDtypeStruct(shape, jnp.float32)
    dma = pltpu.SemaphoreType.DMA
    return pl.pallas_call(
        lambda *refs: coarse_kernel(sections, copies, *refs),
        grid=(1,),
        out_shape=(state, state, state, jax.ShapeDtypeStruct((8, 128), jnp.float32)),
        in_specs=[
            whole, whole, whole, whole, small,
            pl.BlockSpec((1, d), lambda i: (0, 0)),
            pl.BlockSpec((1, d, ff), lambda i: (3, 0, 0)),
            pl.BlockSpec((1, ff, d), lambda i: (3, 0, 0)),
        ],
        out_specs=(whole, whole, whole, small),
        scratch_shapes=[
            pltpu.VMEM(shape, jnp.float32),
            pltpu.VMEM((rounds,) + shape, jnp.float32),
            pltpu.VMEM((2,) + shape, jnp.float32),
            pltpu.VMEM(shape, jnp.bfloat16),
            pltpu.VMEM(shape, jnp.float32),
            pltpu.VMEM((copies, 8, 128), jnp.float32),
            pltpu.VMEM((sections - 1, 8, 128), jnp.float32),
            pltpu.VMEM((8, 128), jnp.float32),
            dma((2,)), dma((rounds,)), dma((2,)),
            dma((copies - 1,)), dma((copies - 1,)),
            dma((sections - 1,)), dma((sections - 1,)),
        ],
        compiler_params=pltpu.CompilerParams(
            collective_id=0, has_side_effects=True, vmem_limit_bytes=40 * 1024 * 1024
        ),
        name="coarse",
    )(initial, start, rhs_one, far_step, tile, gain, first_weights, second_weights)


def local_quads(initial, norm_gains, first_weights, second_weights):
    sections = lax.axis_size("layer")
    here = lax.axis_index("layer")
    place = here % 4
    rows = initial.shape[0]

    def moved(slot, *states):
        stacked = states[0] if len(states) == 1 else jnp.concatenate(states, axis=0)
        return branch(stacked, first_weights[slot], second_weights[slot], norm_gains[slot])

    def near(values):
        return jnp.where(here == 0, initial, shifted(values, "layer", 1))

    def distant(values):
        return jnp.where(here == 3, initial, shifted(values, "layer", 4))

    state = initial
    for slot in range(4):
        state = state + moved(slot, state)
    point = state
    left = near(point)
    far = distant(point)
    state = left
    for slot in range(3):
        state = state + moved(slot, state)
    update = moved(3, state, left, far)
    near_term = update[:rows]
    fine = state + near_term
    rhs_one = fine - (left + 4.0 * update[rows : 2 * rows])
    far_step = far + 16.0 * update[2 * rows :]
    gap = fine - point
    gap_sum = jnp.sum(gap * gap)
    step_sum = jnp.sum(near_term * near_term)

    point = jnp.where(place == 0, fine, point)
    lane = jnp.arange(128)[None, :] == here - 1
    row = jnp.arange(8)[:, None]
    tile = jnp.where(lane & (row == 0), gap_sum, 0.0) + jnp.where(lane & (row == 1), step_sum, 0.0)
    point, left, far, totals = coarse(
        initial, point, rhs_one, far_step, tile, norm_gains[3:4], first_weights, second_weights
    )
    state = left
    states = []
    for slot in range(3):
        state = state + moved(slot, state)
        states.append(state)
    states.append(point)
    lefts = [shifted(s, "layer", 1) for s in states[:3]] + [left]
    fars = [shifted(s, "layer", 4) for s in states[:3]] + [far]
    fours = []
    sixteens = []
    for slot in range(4):
        update = moved(slot, lefts[slot], fars[slot])
        fours.append(states[slot] - (lefts[slot] + 4.0 * update[:rows]))
        sixteens.append(states[slot] - (fars[slot] + 16.0 * update[rows:]))
    points = here * 4 + jnp.arange(4, dtype=jnp.int32) + 1
    defects_four = jnp.where((points >= 4)[:, None, None], jnp.stack(fours), 0.0)
    defects_sixteen = jnp.where((points >= 16)[:, None, None], jnp.stack(sixteens), 0.0)
    gap_total = totals[0, : sections - 1]
    step_total = totals[1, : sections - 1]
    ratios = jnp.sqrt(gap_total / (step_total + epsilon))
    return (jnp.stack(states), ratios, defects_four, defects_sixteen)


def chosen(initial, norm_gains, first_weights, second_weights):
    quads = first_weights.shape[0] == 4 and lax.axis_size("layer") % 4 == 0 and lax.axis_size("dp") > 1
    return (local_quads if quads else local)(initial, norm_gains, first_weights, second_weights)


def solution(mesh):
    placed = (P("dp", None), P("layer", None), P("layer", None, None), P("layer", None, None))
    return jax.shard_map(
        chosen,
        mesh=mesh,
        in_specs=placed,
        out_specs=(P("layer", "dp", None), P(), P("layer", "dp", None), P("layer", "dp", None)),
        check_vma=False,
    )
```

```python
import jax
import jax.numpy as jnp
from jax import lax
from jax.experimental import pallas as pl
from jax.experimental.pallas import tpu as pltpu
from jax.sharding import PartitionSpec as P

epsilon = 1e-06


def shifted(block, axis, distance):
    devices = range(lax.axis_size(axis))
    route = [(i - distance, i) for i in devices if i - distance in devices]
    return lax.ppermute(block, axis, route)


def branch(row_block, weight_in, weight_out, gain_row):
    mean_square = jnp.mean(row_block * row_block, axis=-1, keepdims=True)
    normed = (row_block * lax.rsqrt(mean_square + epsilon) * gain_row).astype(jnp.bfloat16)
    hidden = jax.nn.gelu(
        jnp.dot(normed, weight_in, preferred_element_type=jnp.float32), approximate=True
    ).astype(jnp.bfloat16)
    return jnp.dot(hidden, weight_out, preferred_element_type=jnp.float32)


def local(initial, norm_gains, first_weights, second_weights):
    slot_count = first_weights.shape[0]
    sections = lax.axis_size("layer")
    layer_total = slot_count * sections
    norm_count = layer_total // 4 - 1
    first_point = lax.axis_index("layer") * slot_count
    points = first_point + jnp.arange(slot_count, dtype=jnp.int32) + 1
    spacings = (1, 4, 16)

    def shaped(flags, rank):
        return flags.reshape((slot_count,) + (1,) * (rank - 1))

    def previous(values, level_index):
        spacing = spacings[level_index]
        if spacing >= slot_count:
            portion = values
            distance = spacing // slot_count
        else:
            portion = values[slot_count - spacing :]
            distance = 1
        if level_index == 0:
            arrived = shifted(portion, "layer", distance)
        elif level_index == 1:
            arrived = shifted(portion, "layer", distance)
        else:
            arrived = shifted(portion, "layer", distance)
        if spacing < slot_count:
            arrived = jnp.concatenate([arrived, values[: slot_count - spacing]], axis=0)
        return arrived

    def incoming(values, level_index, anchor):
        arrived = previous(values, level_index)
        from_anchor = shaped(points - spacings[level_index] == 0, values.ndim)
        return jnp.where(from_anchor, anchor, arrived)

    def advance(before, level_index, active, right_side):
        factor = float(spacings[level_index])
        results = []
        for slot in range(slot_count):

            def advance_compute(values, source, slot=slot):
                return (
                    values
                    + factor
                    * branch(values, first_weights[slot], second_weights[slot], norm_gains[slot])
                    + source
                )

            def advance_unchanged(values, source):
                return values

            source = right_side[slot] if right_side is not None else jnp.zeros_like(before[slot])
            results.append(
                lax.cond(active[slot], advance_compute, advance_unchanged, before[slot], source)
            )
        return jnp.stack(results)

    def relaxation(current, level_index, residues, right_side, anchor):
        modulus = 4 * spacings[level_index]
        for residue in residues:
            before = incoming(current, level_index, anchor)
            active = points % modulus == residue
            current = jnp.where(
                shaped(active, 3), advance(before, level_index, active, right_side), current
            )
        return (current, None)

    def restrict(current, level_index, right_side, anchor):
        spacing = spacings[level_index]
        factor = float(spacing)
        wide_factor = float(4 * spacing)
        before = incoming(current, level_index, anchor)
        far_state = incoming(current, level_index + 1, anchor)
        active = points % (4 * spacing) == 0
        row_count = current.shape[1]
        coarse_list = []
        gap_list = []
        step_list = []
        for slot in range(slot_count):

            def restrict_compute(near, distant, held, source, slot=slot):
                update = branch(
                    jnp.concatenate([near, distant], axis=0),
                    first_weights[slot],
                    second_weights[slot],
                    norm_gains[slot],
                )
                near_term = update[:row_count]
                fine_value = near + factor * near_term + source
                coarse = fine_value - (distant + wide_factor * update[row_count:])
                gap = fine_value - held
                return (coarse, jnp.sum(gap * gap), jnp.sum(near_term * near_term))

            def restrict_unchanged(near, distant, held, source):
                nothing = jnp.zeros((), near.dtype)
                return (jnp.zeros_like(near), nothing, nothing)

            source = right_side[slot] if right_side is not None else jnp.zeros_like(before[slot])
            coarse, gap_sum, step_sum = lax.cond(
                active[slot],
                restrict_compute,
                restrict_unchanged,
                before[slot],
                far_state[slot],
                current[slot],
                source,
            )
            coarse_list.append(coarse)
            gap_list.append(gap_sum)
            step_list.append(step_sum)
        return (jnp.stack(coarse_list), jnp.stack(gap_list), jnp.stack(step_list))

    def defects(current, level_index, anchor):
        spacing = spacings[level_index]
        factor = float(spacing)
        before = incoming(current, level_index, anchor)
        stepped = []
        for slot in range(slot_count):
            stepped.append(
                before[slot]
                + factor
                * branch(before[slot], first_weights[slot], second_weights[slot], norm_gains[slot])
            )
        valid = shaped(points >= spacing, 3)
        return jnp.where(valid, current - jnp.stack(stepped), 0.0)

    def multigrid_cycle(anchor):
        current = jnp.broadcast_to(anchor, (slot_count,) + anchor.shape)
        current, unused = relaxation(current, 0, (1, 2, 3), None, anchor)
        current, unused = relaxation(current, 0, (0,), None, anchor)
        current, carried = relaxation(current, 0, (1, 2, 3), None, anchor)
        rhs_one, gap_sums, step_sums = restrict(current, 0, None, anchor)
        current, carried = relaxation(current, 1, (4, 8, 12), rhs_one, anchor)
        rhs_two, unused_gaps, unused_steps = restrict(current, 1, rhs_one, anchor)
        for coarse_step in range(1, layer_total // 16 + 1):
            active = points == 16 * coarse_step
            before = incoming(current, 2, anchor)
            current = jnp.where(shaped(active, 3), advance(before, 2, active, rhs_two), current)
        current, unused = relaxation(current, 1, (4, 8, 12), rhs_one, anchor)
        current, unused = relaxation(current, 0, (1, 2, 3), None, anchor)
        defects_four = defects(current, 1, anchor)
        defects_sixteen = defects(current, 2, anchor)
        return (current, gap_sums, step_sums, defects_four, defects_sixteen)

    portions = [initial]
    outcomes = [multigrid_cycle(portion) for portion in portions]
    layer_states = jnp.concatenate([outcome[0] for outcome in outcomes], axis=1)
    defects_four = jnp.concatenate([outcome[3] for outcome in outcomes], axis=1)
    defects_sixteen = jnp.concatenate([outcome[4] for outcome in outcomes], axis=1)
    gap_sums = outcomes[0][1]
    step_sums = outcomes[0][2]
    counted = (points % 4 == 0) & (points >= 8)
    entry_index = points // 4 - 2
    one_hot = (
        (jnp.arange(norm_count, dtype=jnp.int32)[None, :] == entry_index[:, None])
        & counted[:, None]
    ).astype(jnp.float32)
    gap_vector = jnp.sum(gap_sums[:, None] * one_hot, axis=0)
    step_vector = jnp.sum(step_sums[:, None] * one_hot, axis=0)
    gap_total, step_total = lax.psum((gap_vector, step_vector), ("layer", "dp"))
    residual_ratios = jnp.sqrt(gap_total / (step_total + epsilon))
    return (layer_states, residual_ratios, defects_four, defects_sixteen)


def coarse_kernel(
    sections, copies,
    initial, start, rhs_one, far_step, tile, gain, w_in, w_out,
    point, left, far, totals,
    cur, slots, ends, normed, total, across, along, summed,
    send, arrive, end_arrive, across_send, across_arrive, along_send, along_arrive,
):
    here = lax.axis_index("layer")
    depth = lax.axis_index("dp")
    blocks = sections // 4
    wide_end = blocks + 2
    rounds = wide_end + 2
    ff = w_in.shape[2]
    width = ff // 4

    def to(layer, dp):
        return dict(device_id=(layer, dp), device_id_type=pl.DeviceIdType.MESH)

    cur[...] = start[...]
    across[depth] = tile[...]

    barrier = pltpu.get_barrier_semaphore()
    for k in range(1, sections):
        pl.semaphore_signal(barrier, inc=1, **to(lax.rem(here + k, sections), depth))
    for k in range(1, copies):
        pl.semaphore_signal(barrier, inc=1, **to(here, lax.rem(depth + k, copies)))
    pl.semaphore_wait(barrier, sections + copies - 2)

    def across_copy(k):
        return pltpu.make_async_remote_copy(
            src_ref=tile, dst_ref=across.at[depth],
            send_sem=across_send.at[k - 1], recv_sem=across_arrive.at[k - 1],
            **to(here, lax.rem(depth + k, copies)),
        )

    for k in range(1, copies):
        across_copy(k).start()

    def wide(d, r):
        return (r >= 3) & (r < wide_end) & (d == 4 * (r - 2) + 3)

    def receives(d, r):
        early = (r < 3) & (lax.rem(d, 4) == r + 1)
        middle = (r >= 3) & (r < wide_end) & ((d == 4 * (r - 2)) | (d == 4 * (r - 2) + 3))
        late = (r >= wide_end) & (lax.rem(d, 4) == r - wide_end + 1) & (d >= 4)
        return early | middle | late

    def hop(r, distance):
        return pltpu.make_async_remote_copy(
            src_ref=cur, dst_ref=slots.at[r], send_sem=send.at[distance // 4],
            recv_sem=arrive.at[r], **to(lax.rem(here + distance, sections), depth),
        )

    def step(r, carry):
        one = (here + 1 < sections) & receives(here + 1, r) & jnp.logical_not(wide(here + 1, r))
        four = (here + 4 < sections) & wide(here + 4, r)

        @pl.when(one)
        def _():
            hop(r, 1).start()

        @pl.when(four)
        def _():
            hop(r, 4).start()

        @pl.when(one)
        def _():
            hop(r, 1).wait_send()

        @pl.when(four)
        def _():
            hop(r, 4).wait_send()

        @pl.when(receives(here, r))
        def _():
            hop(r, 1).wait_recv()
            before = slots[r]
            mean_square = jnp.mean(before * before, axis=-1, keepdims=True)
            normed[...] = (before * lax.rsqrt(mean_square + epsilon) * gain[...]).astype(
                jnp.bfloat16
            )
            total[...] = jnp.zeros_like(total)

            def part(i, c):
                cols = pl.ds(pl.multiple_of(i * width, width), width)
                hidden = jax.nn.gelu(
                    jnp.dot(normed[...], w_in[0, :, cols], preferred_element_type=jnp.float32),
                    approximate=True,
                ).astype(jnp.bfloat16)
                total[...] += jnp.dot(
                    hidden, w_out[0, cols, :], preferred_element_type=jnp.float32
                )
                return c

            lax.fori_loop(0, 4, part, 0)
            is_wide = wide(here, r)

            @pl.when(is_wide)
            def _():
                cur[...] = slots[r] + 16.0 * total[...] + (cur[...] - far_step[...])

            @pl.when(jnp.logical_not(is_wide))
            def _():
                cur[...] = slots[r] + 4.0 * total[...] + rhs_one[...]

        return carry

    lax.fori_loop(0, rounds, step, 0)

    def last(distance):
        return pltpu.make_async_remote_copy(
            src_ref=cur, dst_ref=ends.at[distance // 4], send_sem=send.at[distance // 4],
            recv_sem=end_arrive.at[distance // 4],
            **to(lax.rem(here + distance, sections), depth),
        )

    for distance in (1, 4):

        @pl.when(here + distance < sections)
        def _(distance=distance):
            last(distance).start()

    for k in range(1, copies):
        across_copy(k).wait()
    gathered = across[0]
    for k in range(1, copies):
        gathered = gathered + across[k]
    summed[...] = gathered

    def along_copy(k):
        return pltpu.make_async_remote_copy(
            src_ref=summed, dst_ref=along.at[k - 1],
            send_sem=along_send.at[k - 1], recv_sem=along_arrive.at[k - 1],
            **to(lax.rem(here + k, sections), depth),
        )

    for k in range(1, sections):
        along_copy(k).start()
    point[...] = cur[...]
    for distance, out, edge in ((1, left, 1), (4, far, 4)):

        @pl.when(here + distance < sections)
        def _(distance=distance):
            last(distance).wait_send()

        @pl.when(here >= edge)
        def _(distance=distance, out=out):
            last(distance).wait_recv()
            out[...] = ends[distance // 4]

        @pl.when(here < edge)
        def _(out=out):
            out[...] = initial[...]

    result = summed[...]
    for k in range(1, sections):
        along_copy(k).wait()
        result = result + along[k - 1]
    totals[...] = result


def coarse(initial, start, rhs_one, far_step, tile, gain, first_weights, second_weights):
    sections = lax.axis_size("layer")
    copies = lax.axis_size("dp")
    rounds = sections // 4 + 4
    shape = initial.shape
    d, ff = first_weights.shape[1:]
    whole = pl.BlockSpec(shape, lambda i: (0, 0))
    small = pl.BlockSpec((8, 128), lambda i: (0, 0))
    state = jax.ShapeDtypeStruct(shape, jnp.float32)
    dma = pltpu.SemaphoreType.DMA
    return pl.pallas_call(
        lambda *refs: coarse_kernel(sections, copies, *refs),
        grid=(1,),
        out_shape=(state, state, state, jax.ShapeDtypeStruct((8, 128), jnp.float32)),
        in_specs=[
            whole, whole, whole, whole, small,
            pl.BlockSpec((1, d), lambda i: (0, 0)),
            pl.BlockSpec((1, d, ff), lambda i: (3, 0, 0)),
            pl.BlockSpec((1, ff, d), lambda i: (3, 0, 0)),
        ],
        out_specs=(whole, whole, whole, small),
        scratch_shapes=[
            pltpu.VMEM(shape, jnp.float32),
            pltpu.VMEM((rounds,) + shape, jnp.float32),
            pltpu.VMEM((2,) + shape, jnp.float32),
            pltpu.VMEM(shape, jnp.bfloat16),
            pltpu.VMEM(shape, jnp.float32),
            pltpu.VMEM((copies, 8, 128), jnp.float32),
            pltpu.VMEM((sections - 1, 8, 128), jnp.float32),
            pltpu.VMEM((8, 128), jnp.float32),
            dma((2,)), dma((rounds,)), dma((2,)),
            dma((copies - 1,)), dma((copies - 1,)),
            dma((sections - 1,)), dma((sections - 1,)),
        ],
        compiler_params=pltpu.CompilerParams(
            collective_id=0, has_side_effects=True, vmem_limit_bytes=40 * 1024 * 1024
        ),
        name="coarse",
    )(initial, start, rhs_one, far_step, tile, gain, first_weights, second_weights)


def local_quads(initial, norm_gains, first_weights, second_weights):
    sections = lax.axis_size("layer")
    here = lax.axis_index("layer")
    place = here % 4
    rows = initial.shape[0]

    def moved(slot, *states):
        stacked = states[0] if len(states) == 1 else jnp.concatenate(states, axis=0)
        return branch(stacked, first_weights[slot], second_weights[slot], norm_gains[slot])

    def near(values):
        return jnp.where(here == 0, initial, shifted(values, "layer", 1))

    def distant(values):
        return jnp.where(here == 3, initial, shifted(values, "layer", 4))

    state = initial
    for slot in range(4):
        state = state + moved(slot, state)
    point = state
    left = near(point)
    far = distant(point)
    state = left
    for slot in range(3):
        state = state + moved(slot, state)
    update = moved(3, state, left, far)
    near_term = update[:rows]
    fine = state + near_term
    rhs_one = fine - (left + 4.0 * update[rows : 2 * rows])
    far_step = far + 16.0 * update[2 * rows :]
    gap = fine - point
    gap_sum = jnp.sum(gap * gap)
    step_sum = jnp.sum(near_term * near_term)

    point = jnp.where(place == 0, fine, point)
    lane = jnp.arange(128)[None, :] == here - 1
    row = jnp.arange(8)[:, None]
    tile = jnp.where(lane & (row == 0), gap_sum, 0.0) + jnp.where(lane & (row == 1), step_sum, 0.0)
    point, left, far, totals = coarse(
        initial, point, rhs_one, far_step, tile, norm_gains[3:4], first_weights, second_weights
    )
    state = left
    states = []
    for slot in range(3):
        state = state + moved(slot, state)
        states.append(state)
    states.append(point)
    inner = jnp.stack(states[:3])
    lefts = list(shifted(inner, "layer", 1)) + [left]
    fars = list(shifted(inner, "layer", 4)) + [far]
    fours = []
    sixteens = []
    for slot in range(4):
        update = moved(slot, lefts[slot], fars[slot])
        fours.append(states[slot] - (lefts[slot] + 4.0 * update[:rows]))
        sixteens.append(states[slot] - (fars[slot] + 16.0 * update[rows:]))
    points = here * 4 + jnp.arange(4, dtype=jnp.int32) + 1
    defects_four = jnp.where((points >= 4)[:, None, None], jnp.stack(fours), 0.0)
    defects_sixteen = jnp.where((points >= 16)[:, None, None], jnp.stack(sixteens), 0.0)
    gap_total = totals[0, : sections - 1]
    step_total = totals[1, : sections - 1]
    ratios = jnp.sqrt(gap_total / (step_total + epsilon))
    return (jnp.stack(states), ratios, defects_four, defects_sixteen)


def chosen(initial, norm_gains, first_weights, second_weights):
    quads = first_weights.shape[0] == 4 and lax.axis_size("layer") % 4 == 0 and lax.axis_size("dp") > 1
    return (local_quads if quads else local)(initial, norm_gains, first_weights, second_weights)


def solution(mesh):
    placed = (P("dp", None), P("layer", None), P("layer", None, None), P("layer", None, None))
    return jax.shard_map(
        chosen,
        mesh=mesh,
        in_specs=placed,
        out_specs=(P("layer", "dp", None), P(), P("layer", "dp", None), P("layer", "dp", None)),
        check_vma=False,
    )
```
